32 devices in a mesh: dp: 16 (over z, x, core), tp: 2 (over y).
Axes of the slice: x: 2, y: 2, z: 4, core: 2. Of those that a mesh axis runs over, the one named last changes fastest.
Arguments:
- queries: bfloat16 [128, 8192], P('dp', 'tp'), may hold values from -5 to 5
- prefix_kv: bfloat16 [2, 32768, 1024], P(None, 'dp', 'tp'), may hold values from -5 to 5
- cache_kv: bfloat16 [2, 1024, 64, 1024], P(None, 'dp', None, 'tp'), may hold values from -5 to 5
- lengths: int32 [128], P('dp'), may hold values from 1 to 512, as said below
- page_table: int32 [16, 64], P('dp'), may hold values from 0 to 63, each once within a row
- owner: int32 [16], replicated, may hold values from 0 to 15, as said below
- readers: int32 [8], replicated, may hold values from 0 to 15, as said below
- w_out: bfloat16 [8192, 4096], P('tp'), may hold values from -0.5 to 0.5
Outputs:
- projected: bfloat16 [128, 4096], P('dp', 'tp')
The draws below stay inside these ranges and needn't reach their ends.
Inputs may be any that keep to these rules, and one draw needn't show every extreme that they name: `lengths`: at most 512, reached by some request in every draw. `page_table`: each row holds every page id of its replica once. `owner`: every replica index once. `readers`: 8 distinct replica indices, none of them owner[0].
All inputs are finite; a program needn't handle non-finite values.
Results may differ from the reference program's by a relative error of at most 0.0051.
Values may be sent and summed in bfloat16 or wider, within the bound.
No kernel may reach another device: no remote copies, remote signals or barrier semaphores. Data moves between devices by JAX's collectives and lax.ppermute only.
A program may use at most 128 MiB of HBM per device.

```python
import jax
import jax.numpy as jnp
from jax import lax

HEADS = 64
KV_HEADS = 8
HD = 128
D_OUT = 4096
PREFIX = 2048
PAGE = 64
MAXLEN = 512
B = 8
NPAGES = 64
READERS = 8
N_DP = 16


def draw_queries(key, part):
    rows = N_DP * B
    values = jnp.clip(2.0 * jax.random.normal(jax.random.fold_in(key, 23), (rows, HEADS, HD), jnp.float32), -5.0, 5.0)
    return values.reshape(rows, HEADS * HD).astype(jnp.bfloat16)


def draw_cache_kv(key, part):
    shape = (2, N_DP * NPAGES, PAGE, KV_HEADS, HD)
    values = jnp.clip(jax.random.normal(jax.random.fold_in(key, 32), shape, jnp.float32), -5.0, 5.0)
    return values.reshape(2, N_DP * NPAGES, PAGE, KV_HEADS * HD).astype(jnp.bfloat16)


def draw_lengths(key, part):
    caps = jax.random.randint(jax.random.fold_in(key, 41), (N_DP, 1), MAXLEN // 4, MAXLEN + 1)
    raw = jax.random.randint(jax.random.fold_in(key, 42), (N_DP, B), 0, 1 << 20)
    lens = 1 + raw % caps
    chosen = jax.random.randint(jax.random.fold_in(key, 43), (), 0, N_DP)
    lens = lens.at[chosen, 0].set(MAXLEN)
    return lens.reshape(N_DP * B).astype(jnp.int32)


def owner_and_readers(key):
    ranking = jax.random.permutation(jax.random.fold_in(key, 61), N_DP).astype(jnp.int32)
    first = ranking[0]
    offsets = jnp.arange(1, N_DP, dtype=jnp.int32)
    tier = jnp.where(offsets == 1, 3, jnp.where(offsets == N_DP // 2, 2, jnp.where(offsets == N_DP - 1, 1, 0)))
    noise = jax.random.randint(jax.random.fold_in(key, 62), (N_DP - 1,), 0, 1024)
    scores = (tier * 1024 + noise) * N_DP + offsets
    _, picked = lax.top_k(scores, READERS)
    chosen = offsets[picked]
    readers = (first + chosen) % N_DP
    return (ranking, readers.astype(jnp.int32))


def draw_owner(key, part):
    return owner_and_readers(key)[0]


def draw_readers(key, part):
    return owner_and_readers(key)[1]


def with_spikes(values, stream_key, source, target, blocks, factor):
    def block_of(dim):
        return (jnp.arange(values.shape[dim]) // (values.shape[dim] // blocks)).reshape((-1,) + (1,) * (values.ndim - 1 - dim))

    one_side = jax.random.permutation(stream_key, blocks)[block_of(target)]
    other_side = (block_of(target) + blocks // 2) % blocks
    return jnp.where((block_of(source) == one_side) | (block_of(source) == other_side), factor * values, values)


def steps_of(rng, extent, shards, least, high):
    factor_of = 1.0
    for position, blocks in shards:
        heights = jax.random.uniform(jax.random.fold_in(jax.random.fold_in(rng, 6), position), (blocks,), jnp.float32, least / len(shards), high / len(shards))
        factor_of = factor_of * jnp.repeat(jnp.exp(heights), extent[position] // blocks).reshape((-1,) + (1,) * (len(extent) - 1 - position))
    return factor_of


def normal_values(own_key, extent, deviation, reach, shards=(), kind=jnp.bfloat16):
    result = deviation * jax.random.normal(own_key, extent, jnp.float32)
    if shards:
        result = result * steps_of(own_key, extent, shards, -0.22, 0.18)
    return jnp.clip(result, -reach, reach).astype(kind)


def bell_draw_with(key, dims, spread, limit, split, heavy, held_as=jnp.bfloat16):
    values = spread * jax.random.normal(key, dims, jnp.float32)
    if split:
        values = values * steps_of(key, dims, split, -0.22, 0.18)
    return jnp.clip(with_spikes(values, jax.random.fold_in(key, 3), *heavy), -limit, limit).astype(held_as)


def setup_inputs(seed: int = 0) -> dict:
    key_list = jax.random.split(jax.random.key(seed), 9)
    return {
        "queries": draw_queries(jax.random.fold_in(key_list[8], 71), 0),
        "prefix_kv": normal_values(key_list[1], (2, N_DP * PREFIX, KV_HEADS * HD), 1.0, 5.0, ((1, 16), (2, 2))),
        "cache_kv": draw_cache_kv(jax.random.fold_in(key_list[8], 71), 0),
        "lengths": draw_lengths(jax.random.fold_in(key_list[8], 71), 0),
        "page_table": jax.vmap(lambda own: jax.random.permutation(own, NPAGES))(jax.random.split(key_list[4], N_DP)).reshape((N_DP, NPAGES)).astype(jnp.int32),
        "owner": draw_owner(jax.random.fold_in(key_list[8], 71), 0),
        "readers": draw_readers(jax.random.fold_in(key_list[8], 71), 0),
        "w_out": bell_draw_with(key_list[7], (HEADS * HD, D_OUT), 0.08, 0.5, ((0, 2),), (0, 1, 2, 2.0)),
    }


def reference(queries, prefix_kv, cache_kv, lengths, page_table, owner, readers, w_out):
    group = HEADS // KV_HEADS
    maxpages = MAXLEN // PAGE
    scale = 1.0 / (HD ** 0.5)
    start = (owner[0] * PREFIX).astype(jnp.int32)
    prefix = lax.dynamic_slice_in_dim(prefix_kv, start, PREFIX, 1)
    prefix = prefix.reshape(2, PREFIX, KV_HEADS, HD).astype(jnp.float32)
    replicas = jnp.arange(N_DP, dtype=jnp.int32)
    flags = jnp.any(readers[None, :] == replicas[:, None], axis=1)

    def replica(index):
        first = (index * B).astype(jnp.int32)
        query = lax.dynamic_slice_in_dim(queries, first, B, 0)
        query = query.reshape(B, KV_HEADS, group, HD).astype(jnp.float32)
        pages = page_table[index].reshape(B, maxpages) + index * NPAGES
        resident = cache_kv[:, pages].reshape(2, B, MAXLEN, KV_HEADS, HD).astype(jnp.float32)
        lens = lax.dynamic_slice_in_dim(lengths, first, B, 0)
        s_res = jnp.einsum("bkgd,btkd->bkgt", query, resident[0]) * scale
        inside = jnp.arange(MAXLEN, dtype=jnp.int32)[None, :] < lens[:, None]
        s_res = jnp.where(inside[:, None, None, :], s_res, -jnp.inf)
        s_pre = jnp.einsum("bkgd,tkd->bkgt", query, prefix[0]) * scale
        s_pre = jnp.where(flags[index], s_pre, -jnp.inf)
        top = jnp.maximum(jnp.max(s_res, axis=-1), jnp.max(s_pre, axis=-1))
        e_res = jnp.exp(s_res - top[..., None])
        e_pre = jnp.exp(s_pre - top[..., None])
        den = jnp.sum(e_res, axis=-1) + jnp.sum(e_pre, axis=-1)
        r_res = lax.optimization_barrier(e_res.astype(jnp.bfloat16)).astype(jnp.float32)
        r_pre = lax.optimization_barrier(e_pre.astype(jnp.bfloat16)).astype(jnp.float32)
        num = jnp.einsum("bkgt,btkd->bkgd", r_res, resident[1]) + jnp.einsum("bkgt,tkd->bkgd", r_pre, prefix[1])
        return (num / den[..., None]).astype(jnp.bfloat16).reshape(B, HEADS * HD)

    attn = lax.map(replica, replicas).reshape(N_DP * B, HEADS * HD)
    return jnp.dot(attn, w_out, preferred_element_type=jnp.float32).astype(jnp.bfloat16)
```

```python
import functools

import jax
import jax.numpy as jnp
from jax import lax
from jax.experimental import pallas as pl
from jax.experimental.pallas import tpu as pltpu
from jax.sharding import PartitionSpec as P


HD = 128
PAGE = 64
LOG2E = 1.4426950408889634
VMEM = pltpu.VMEM
SMEM = pltpu.SMEM


def vmem_spec():
    return pl.BlockSpec(memory_space=VMEM)


def smem_spec():
    return pl.BlockSpec(memory_space=SMEM)


def hbm_spec():
    return pl.BlockSpec(memory_space=pltpu.HBM)


def in_hbm(x):
    return pltpu.with_memory_space_constraint(x, pltpu.HBM)


def place():
    return lax.axis_index("dp").astype(jnp.int32)


def split_kernel(half, q_ref, mine, other):
    core = lax.rem(place(), 2)
    mine[...] = q_ref[:, pl.ds(pl.multiple_of(core * half, 128), half)]
    other[...] = q_ref[:, pl.ds(pl.multiple_of((1 - core) * half, 128), half)]


def pair_kernel(mine, got, after, out):
    out[0] = mine[...]
    out[1] = got[...]


def share_kernel(cols, kv, after, out, sem):
    side = 1 - lax.rem(place(), 2) if kv.shape[2] > cols else 0
    copy = pltpu.make_async_copy(kv.at[:, :, pl.ds(pl.multiple_of(side * cols, 128), cols)], out, sem)
    copy.start()
    copy.wait()


def w_copies(plan, first, w, outs, sems):
    n_tp, chunk, width = plan
    per_chunk = chunk // width
    my_tp = lax.axis_index("tp").astype(jnp.int32)
    copies = []
    for i, out in enumerate(outs):
        which, block = divmod(first + i, per_chunk)
        col = jnp.bitwise_xor(my_tp, (which + 1) % n_tp) * chunk + block * width
        copies.append(pltpu.make_async_copy(w.at[:, pl.ds(pl.multiple_of(col, 128), width)], out, sems.at[i]))
    return copies


def choose_kernel(chips, owner, *refs):
    parts, near, far = refs[:chips], refs[chips], refs[chips + 1]
    source = jnp.bitwise_xor(place() // 2, owner[0] // 2)
    for d in range(chips):

        @pl.when(source == d)
        def _():
            near[...] = parts[d][0]
            far[...] = parts[d][1]


def resident_kernel(rows, groups, group, maxpages, plan, count, table, lengths, q_ref, cache, kv, w, *refs):
    out, lse_out, own = refs[:3]
    kbuf, vbuf, sems, own_sem, w_sems = refs[3 + count :]
    length = maxpages * PAGE
    scale = 1.0 / HD**0.5
    for kind, buf in ((0, kbuf), (1, vbuf)):
        for b in range(rows):
            for t in range(maxpages):
                pltpu.make_async_copy(
                    cache.at[kind, table[b * maxpages + t]], buf.at[b, t], sems.at[kind, b]
                ).start()
    cols = own.shape[2]
    part = lax.rem(place(), 2) if kv.shape[2] > cols else 0
    own_copy = pltpu.make_async_copy(kv.at[:, :, pl.ds(pl.multiple_of(part * cols, 128), cols)], own, own_sem)
    own_copy.start()
    w_parts = w_copies(plan, 0, w, refs[3 : 3 + count], w_sems)
    for copy in w_parts:
        copy.start()
    m_rows = group * rows
    row_b = lax.rem(lax.broadcasted_iota(jnp.int32, (m_rows, 1), 0), rows)
    lens = jnp.zeros((m_rows, 1), jnp.int32)
    for b in range(rows):
        lens = jnp.where(row_b == b, lengths[b], lens)
    inside = lax.broadcasted_iota(jnp.int32, (m_rows, length), 1) < lens
    for b in range(rows):
        pltpu.make_async_copy(cache.at[0, pl.ds(0, maxpages)], kbuf.at[b], sems.at[0, b]).wait()
    probs = []
    stats = []
    for g in range(groups):
        qs = [q_ref[:, (g * group + h) * HD : (g * group + h + 1) * HD].astype(jnp.float32) for h in range(group)]
        qg = jnp.concatenate(qs, axis=0).astype(jnp.bfloat16)
        s = None
        for b in range(rows):
            kb = kbuf[b, :, :, g * HD : (g + 1) * HD].reshape(length, HD)
            sb = lax.dot_general(qg, kb, (((1,), (1,)), ((), ())), preferred_element_type=jnp.float32)
            s = sb if s is None else jnp.where(row_b == b, sb, s)
        s = jnp.where(inside, s, -jnp.inf)
        top = jnp.max(s, axis=1, keepdims=True)
        p = jnp.exp2((s - top) * (scale * LOG2E))
        den = jnp.sum(p, axis=1, keepdims=True)
        probs.append(p.astype(jnp.bfloat16))
        stats.append((1.0 / den, top * scale + jnp.log(den)))
    for b in range(rows):
        pltpu.make_async_copy(cache.at[1, pl.ds(0, maxpages)], vbuf.at[b], sems.at[1, b]).wait()
    half_heads = groups * group // 2
    lane = lax.broadcasted_iota(jnp.int32, (rows, 128), 1)
    lse = [jnp.zeros((rows, 128), jnp.float32) for _ in range(2)]
    for g in range(groups):
        o = None
        for b in range(rows):
            vb = vbuf[b, :, :, g * HD : (g + 1) * HD].reshape(length, HD)
            ob = jnp.dot(probs[g], vb, preferred_element_type=jnp.float32)
            o = ob if o is None else jnp.where(row_b == b, ob, o)
        inv, lg = stats[g]
        o = o * inv
        for h in range(group):
            side, hh = divmod(g * group + h, half_heads)
            out[side, :, hh * HD : (hh + 1) * HD] = o[h * rows : (h + 1) * rows, :]
            lse[side] = jnp.where(lane == hh, lg[h * rows : (h + 1) * rows, :], lse[side])
    for side in range(2):
        lse_out[side] = lse[side]
    own_copy.wait()
    for copy in w_parts:
        copy.wait()


def prefix_kernel(chips, rows, groups, group, n_readers, block, plan, first_w, count, owner_ref, readers, *refs):
    q_refs = refs[:chips]
    own_kv, mate_kv, w = refs[chips : chips + 3]
    outs, w_dst = refs[chips + 3 : 2 * chips + 3], refs[2 * chips + 3 : 2 * chips + 3 + count]
    q_all, q_rows, o_rows, lse_rows, o_all, w_sems = refs[2 * chips + 3 + count :]
    w_parts = w_copies(plan, first_w, w, w_dst, w_sems)
    for copy in w_parts:
        copy.start()
    me, owner = place(), owner_ref[0]
    scale = 1.0 / HD**0.5
    half = groups * group * HD

    @pl.when(me // 2 == owner // 2)
    def _():
        for d in range(chips):
            for s in range(2):
                q_all[2 * d + s] = q_refs[d][s].astype(jnp.float32)
        for j in range(n_readers):
            slot = jnp.bitwise_xor(readers[j], me)
            x = q_all[slot]
            for g in range(groups):
                for h in range(group):
                    first = (h * n_readers + j) * rows
                    col = (g * group + h) * HD
                    q_rows[g, first : first + rows, :] = x[:, col : col + HD]
        total = group * n_readers * rows
        blocks = total // block

        def attend(kv):
            for g in range(groups):

                @pl.loop(0, blocks)
                def _(i):
                    part = pl.ds(pl.multiple_of(i * block, block), block)
                    q = q_rows[g, part, :].astype(jnp.bfloat16)
                    keys = kv[0, :, g * HD : (g + 1) * HD]
                    s = lax.dot_general(q, keys, (((1,), (1,)), ((), ())), preferred_element_type=jnp.float32)
                    top = jnp.max(s, axis=1, keepdims=True)
                    p = jnp.exp2((s - top) * (scale * LOG2E))
                    den = jnp.sum(p, axis=1, keepdims=True)
                    values = kv[1, :, g * HD : (g + 1) * HD]
                    o = jnp.dot(p.astype(jnp.bfloat16), values, preferred_element_type=jnp.float32)
                    o_rows[g, part, :] = o * (1.0 / den)
                    lse_rows[g, part, :] = jnp.broadcast_to(top * scale + jnp.log(den), (block, 128))

        @pl.when(me == owner)
        def _():
            attend(own_kv)

        @pl.when(me != owner)
        def _():
            attend(mate_kv)

        lane = lax.broadcasted_iota(jnp.int32, (rows, 128), 1)
        heads = groups * group
        for j in range(n_readers):
            slot = jnp.bitwise_xor(readers[j], me)
            stat = jnp.zeros((rows, 128), jnp.float32)
            for g in range(groups):
                for h in range(group):
                    first = (h * n_readers + j) * rows
                    hh = g * group + h
                    o_all[slot, :, hh * HD : (hh + 1) * HD] = o_rows[g, first : first + rows, :]
                    val = lse_rows[g, first : first + rows, :]
                    top = val.astype(jnp.bfloat16).astype(jnp.float32)
                    rest = val - top
                    mid = rest.astype(jnp.bfloat16).astype(jnp.float32)
                    stat = jnp.where(lane == hh, top, stat)
                    stat = jnp.where(lane == heads + hh, mid, stat)
                    stat = jnp.where(lane == 2 * heads + hh, rest - mid, stat)
            o_all[slot, :, half:] = stat
        for d in range(chips):
            for s in range(2):
                outs[d][s] = o_all[2 * d + s].astype(jnp.bfloat16)

    for copy in w_parts:
        copy.wait()


def project(attn, w, outs, first, width):
    per_chunk = outs[0].shape[1] // width
    for i, out in enumerate(outs):
        for j in range(per_chunk):
            block = w[first + i * per_chunk + j]
            out[:, j * width : (j + 1) * width] = jnp.dot(attn, block[...], preferred_element_type=jnp.float32)


def away_kernel(heads, plan, loaded, later, readers, near, far, res, res_lse, w_hbm, *refs):
    n_tp, chunk, width = plan
    w, outs, attn, w_dst, w_sems = (
        refs[:loaded],
        refs[loaded : loaded + n_tp - 1],
        refs[loaded + n_tp - 1],
        refs[loaded + n_tp : loaded + n_tp + later],
        refs[-1],
    )
    copies = w_copies(plan, n_tp * (chunk // width) - later, w_hbm, w_dst, w_sems)
    for copy in copies:
        copy.start()
    me = place()
    core = lax.rem(me, 2)
    is_reader = jnp.int32(0)
    for j in range(readers.shape[0]):
        is_reader = jnp.where(readers[j] == me, 1, is_reader)
    half = heads * HD
    for side in range(2):
        mine = core == side
        stat = jnp.where(mine, near[:, half:], far[:, half:]).astype(jnp.float32)
        r_lse = res_lse[side]
        for h in range(heads):
            pre = (
                stat[:, h : h + 1] + stat[:, heads + h : heads + h + 1] + stat[:, 2 * heads + h : 2 * heads + h + 1]
            )
            weight = 1.0 / (1.0 + jnp.exp(r_lse[:, h : h + 1] - pre))
            cols = slice(h * HD, (h + 1) * HD)
            r = res[side, :, cols]
            x = jnp.where(mine, near[:, cols].astype(jnp.float32), far[:, cols].astype(jnp.float32))
            y = jnp.where(is_reader > 0, r + weight * (x - r), r)
            attn[:, side * half + h * HD : side * half + (h + 1) * HD] = y.astype(jnp.bfloat16)
    project(attn[...], w, outs, 0, width)
    for copy in copies:
        copy.wait()


def home_kernel(width, attn, *refs):
    project(attn[...], refs[:-1], refs[-1:], 0, width)


def shards(n_dp, n_tp, queries, prefix_kv, cache_kv, lengths, page_table, owner, readers, w_out):
    rows = queries.shape[0]
    heads = queries.shape[1] // HD
    groups = prefix_kv.shape[2] // HD
    group = heads // groups
    prefix = prefix_kv.shape[1]
    maxpages = page_table.shape[1] // rows
    n_readers = readers.shape[0]
    chips = n_dp // 2
    half_groups = max(groups // 2, 1)
    half_heads = heads // 2
    share_group = half_heads // half_groups
    half = half_heads * HD
    wide = half + 128
    d_out = w_out.shape[1]
    chunk = d_out // n_tp

    def hop(x, d):
        return lax.ppermute(x, "dp", [(i, i ^ d) for i in range(n_dp)])

    mine, other = pl.pallas_call(
        functools.partial(split_kernel, half),
        out_shape=tuple(jax.ShapeDtypeStruct((rows, half), jnp.bfloat16) for _ in range(2)),
        in_specs=[vmem_spec()],
        out_specs=(vmem_spec(), vmem_spec()),
        compiler_params=pltpu.CompilerParams(vmem_limit_bytes=2 << 20),
        name="split",
    )(queries)
    got = hop(other, 1)
    kv_cols = half_groups * HD
    shared = pl.pallas_call(
        functools.partial(share_kernel, kv_cols),
        out_shape=jax.ShapeDtypeStruct((2, prefix, kv_cols), jnp.bfloat16),
        in_specs=[hbm_spec(), vmem_spec()],
        out_specs=vmem_spec(),
        scratch_shapes=[pltpu.SemaphoreType.DMA(())],
        compiler_params=pltpu.CompilerParams(vmem_limit_bytes=4 << 20),
        cost_estimate=pl.CostEstimate(flops=1 << 24, bytes_accessed=4 * prefix * kv_cols, transcendentals=0),
        name="share",
    )(in_hbm(prefix_kv), other)
    pair = pl.pallas_call(
        pair_kernel,
        out_shape=jax.ShapeDtypeStruct((2, rows, half), jnp.bfloat16),
        in_specs=[vmem_spec()] * 3,
        out_specs=vmem_spec(),
        compiler_params=pltpu.CompilerParams(vmem_limit_bytes=2 << 20),
        cost_estimate=pl.CostEstimate(flops=1 << 32, bytes_accessed=1 << 24, transcendentals=0),
        name="pair",
    )(mine, got, shared)
    mate_kv = hop(shared, 1)
    gathered = [pair] + [hop(pair, 2 * d) for d in range(1, chips)]

    m_rows = group * rows
    width = min(512, chunk)
    plan = (n_tp, chunk, width)
    last = min(2, chunk // width)
    counts = (1, d_out // width - 1 - last, last)

    def w_outs(n):
        return tuple(VMEM((w_out.shape[0], width), w_out.dtype) for _ in range(n))

    res, res_lse, own_kv, *w_parts = pl.pallas_call(
        functools.partial(resident_kernel, rows, groups, group, maxpages, plan, counts[0]),
        out_shape=(
            jax.ShapeDtypeStruct((2, rows, half), jnp.float32),
            jax.ShapeDtypeStruct((2, rows, 128), jnp.float32),
            jax.ShapeDtypeStruct((2, prefix, kv_cols), jnp.bfloat16),
        )
        + w_outs(counts[0]),
        in_specs=[smem_spec(), smem_spec(), vmem_spec(), hbm_spec(), hbm_spec(), hbm_spec()],
        out_specs=(vmem_spec(),) * (3 + counts[0]),
        scratch_shapes=[
            VMEM((rows, maxpages, PAGE, groups * HD), jnp.bfloat16),
            VMEM((rows, maxpages, PAGE, groups * HD), jnp.bfloat16),
            pltpu.SemaphoreType.DMA((2, rows)),
            pltpu.SemaphoreType.DMA(()),
            pltpu.SemaphoreType.DMA((counts[0],)),
        ],
        compiler_params=pltpu.CompilerParams(vmem_limit_bytes=13 << 20),
        cost_estimate=pl.CostEstimate(
            flops=4 * heads * rows * rows * maxpages * PAGE * HD,
            bytes_accessed=2 * rows * maxpages * PAGE * groups * HD * 2,
            transcendentals=groups * m_rows * maxpages * PAGE,
        ),
        name="resident",
    )(page_table[0], lengths, queries, in_hbm(cache_kv), in_hbm(prefix_kv), in_hbm(w_out))

    total = share_group * n_readers * rows
    block = min(256, total)
    pre = pl.pallas_call(
        functools.partial(
            prefix_kernel, chips, rows, half_groups, share_group, n_readers, block, plan, counts[0], counts[1]
        ),
        out_shape=tuple(jax.ShapeDtypeStruct((2, rows, wide), jnp.bfloat16) for _ in range(chips))
        + w_outs(counts[1]),
        in_specs=[smem_spec(), smem_spec()] + [vmem_spec()] * (chips + 2) + [hbm_spec()],
        out_specs=(vmem_spec(),) * (chips + counts[1]),
        scratch_shapes=[
            VMEM((2 * chips, rows, half), jnp.float32),
            VMEM((half_groups, total, HD), jnp.float32),
            VMEM((half_groups, total, HD), jnp.float32),
            VMEM((half_groups, total, 128), jnp.float32),
            VMEM((2 * chips, rows, wide), jnp.float32),
            pltpu.SemaphoreType.DMA((counts[1],)),
        ],
        compiler_params=pltpu.CompilerParams(vmem_limit_bytes=12 << 20),
        cost_estimate=pl.CostEstimate(
            flops=4 * half_groups * total * prefix * HD,
            bytes_accessed=4 * half_groups * prefix * HD,
            transcendentals=half_groups * total * prefix,
        ),
        name="prefix",
    )(owner, readers, *gathered, own_kv, mate_kv, in_hbm(w_out))
    w_parts = [pltpu.with_memory_space_constraint(x, VMEM) for x in list(w_parts) + list(pre[chips:])]

    back = [pre[0]] + [hop(pre[d], 2 * d) for d in range(1, chips)]
    near, other = pl.pallas_call(
        functools.partial(choose_kernel, chips),
        out_shape=tuple(jax.ShapeDtypeStruct((rows, wide), jnp.bfloat16) for _ in range(2)),
        in_specs=[smem_spec()] + [vmem_spec()] * chips,
        out_specs=(vmem_spec(), vmem_spec()),
        compiler_params=pltpu.CompilerParams(vmem_limit_bytes=4 << 20),
        name="choose",
    )(owner, *back)
    far = hop(other, 1)


    per_chunk = chunk // width
    cost = pl.CostEstimate(
        flops=2 * rows * heads * HD * chunk * 16, bytes_accessed=2 * heads * HD * chunk, transcendentals=0
    )
    projected = pl.pallas_call(
        functools.partial(away_kernel, half_heads, plan, len(w_parts), counts[2]),
        out_shape=tuple(jax.ShapeDtypeStruct((rows, chunk), jnp.float32) for _ in range(n_tp - 1))
        + (jax.ShapeDtypeStruct((rows, heads * HD), jnp.bfloat16),)
        + w_outs(counts[2]),
        in_specs=[smem_spec()] + [vmem_spec()] * 4 + [hbm_spec()] + [vmem_spec()] * len(w_parts),
        out_specs=(vmem_spec(),) * (n_tp + counts[2]),
        scratch_shapes=[pltpu.SemaphoreType.DMA((counts[2],))],
        compiler_params=pltpu.CompilerParams(vmem_limit_bytes=4 << 20),
        cost_estimate=cost,
        name="away",
    )(readers, near, far, res, res_lse, in_hbm(w_out), *w_parts)
    away, attn = projected[: n_tp - 1], projected[n_tp - 1]
    w_parts = (w_parts + list(projected[n_tp:]))[-per_chunk:]
    home = pl.pallas_call(
        functools.partial(home_kernel, width),
        out_shape=jax.ShapeDtypeStruct((rows, chunk), jnp.float32),
        in_specs=[vmem_spec()] * (1 + per_chunk),
        out_specs=vmem_spec(),
        compiler_params=pltpu.CompilerParams(vmem_limit_bytes=4 << 20),
        cost_estimate=cost,
        name="home",
    )(attn, *w_parts)
    for k in range(1, n_tp):
        home = home + lax.ppermute(away[k - 1], "tp", [(i, i ^ k) for i in range(n_tp)])
    return home.astype(jnp.bfloat16)


def solution(mesh):
    placed = (
        P("dp", "tp"),
        P(None, "dp", "tp"),
        P(None, "dp", None, "tp"),
        P("dp"),
        P("dp", None),
        P(),
        P(),
        P("tp", None),
    )
    return jax.shard_map(
        functools.partial(shards, mesh.shape["dp"], mesh.shape["tp"]),
        mesh=mesh,
        in_specs=placed,
        out_specs=P("dp", "tp"),
        check_vma=False,
    )
```

```python
import functools

import jax
import jax.numpy as jnp
from jax import lax
from jax.experimental import pallas as pl
from jax.experimental.pallas import tpu as pltpu
from jax.sharding import PartitionSpec as P


HD = 128
PAGE = 64
LOG2E = 1.4426950408889634
VMEM = pltpu.VMEM
SMEM = pltpu.SMEM


def vmem_spec():
    return pl.BlockSpec(memory_space=VMEM)


def smem_spec():
    return pl.BlockSpec(memory_space=SMEM)


def hbm_spec():
    return pl.BlockSpec(memory_space=pltpu.HBM)


def in_hbm(x):
    return pltpu.with_memory_space_constraint(x, pltpu.HBM)


def place():
    return lax.axis_index("dp").astype(jnp.int32)


def split_kernel(half, q_ref, mine, other):
    core = lax.rem(place(), 2)
    mine[...] = q_ref[:, pl.ds(pl.multiple_of(core * half, 128), half)]
    other[...] = q_ref[:, pl.ds(pl.multiple_of((1 - core) * half, 128), half)]


def pair_kernel(mine, got, after, out):
    out[0] = mine[...]
    out[1] = got[...]


def share_kernel(cols, kv, after, out, sem):
    side = 1 - lax.rem(place(), 2) if kv.shape[2] > cols else 0
    copy = pltpu.make_async_copy(kv.at[:, :, pl.ds(pl.multiple_of(side * cols, 128), cols)], out, sem)
    copy.start()
    copy.wait()


def w_copies(plan, first, w, outs, sems):
    n_tp, chunk, width = plan
    per_chunk = chunk // width
    my_tp = lax.axis_index("tp").astype(jnp.int32)
    copies = []
    for i in range(outs.shape[0]):
        which, block = divmod(first + i, per_chunk)
        col = jnp.bitwise_xor(my_tp, (which + 1) % n_tp) * chunk + block * width
        copies.append(pltpu.make_async_copy(w.at[:, pl.ds(pl.multiple_of(col, 128), width)], outs.at[i], sems.at[i]))
    return copies


def load_kernel(plan, w, after, out, token, sems):
    copies = w_copies(plan, 0, w, out, sems)
    for copy in copies:
        copy.start()
    for copy in copies:
        copy.wait()
    token[...] = jnp.zeros_like(token)


def choose_kernel(chips, owner, *refs):
    parts, near, far = refs[:chips], refs[chips + 1], refs[chips + 2]
    source = jnp.bitwise_xor(place() // 2, owner[0] // 2)
    for d in range(chips):

        @pl.when(source == d)
        def _():
            near[...] = parts[d][0]
            far[...] = parts[d][1]


def resident_kernel(
    rows, groups, group, maxpages, table, lengths, q_ref, cache, out, lse_out, kbuf, vbuf, sems
):
    length = maxpages * PAGE
    scale = 1.0 / HD**0.5
    for kind, buf in ((0, kbuf), (1, vbuf)):
        for b in range(rows):
            for t in range(maxpages):
                pltpu.make_async_copy(
                    cache.at[kind, table[b * maxpages + t]], buf.at[b, t], sems.at[kind, b]
                ).start()
    m_rows = group * rows
    row_b = lax.rem(lax.broadcasted_iota(jnp.int32, (m_rows, 1), 0), rows)
    lens = jnp.zeros((m_rows, 1), jnp.int32)
    for b in range(rows):
        lens = jnp.where(row_b == b, lengths[b], lens)
    inside = lax.broadcasted_iota(jnp.int32, (m_rows, length), 1) < lens
    half_heads = groups * group // 2
    lane = lax.broadcasted_iota(jnp.int32, (rows, 128), 1)
    lse_out[...] = jnp.zeros_like(lse_out)

    def arrived(kind, buf):
        for b in range(rows):
            pltpu.make_async_copy(cache.at[kind, pl.ds(0, maxpages)], buf.at[b], sems.at[kind, b]).wait()

    arrived(0, kbuf)

    @pl.loop(0, groups)
    def _(g):
        kv_cols = pl.ds(pl.multiple_of(g * HD, HD), HD)
        q_cols = pl.ds(pl.multiple_of(g * group * HD, group * HD), group * HD)
        q = q_ref[:, q_cols].astype(jnp.float32)
        q = jnp.concatenate([q[:, h * HD : (h + 1) * HD] for h in range(group)], axis=0).astype(jnp.bfloat16)
        s = None
        for b in range(rows):
            keys = kbuf[b, :, :, kv_cols].reshape(length, HD)
            sb = lax.dot_general(q, keys, (((1,), (1,)), ((), ())), preferred_element_type=jnp.float32)
            s = sb if s is None else jnp.where(row_b == b, sb, s)
        s = jnp.where(inside, s, -jnp.inf)
        top = jnp.max(s, axis=1, keepdims=True)
        p = jnp.exp2((s - top) * (scale * LOG2E))
        den = jnp.sum(p, axis=1, keepdims=True)
        p = p.astype(jnp.bfloat16)

        @pl.when(g == 0)
        def _():
            arrived(1, vbuf)

        o = None
        for b in range(rows):
            values = vbuf[b, :, :, kv_cols].reshape(length, HD)
            ob = jnp.dot(p, values, preferred_element_type=jnp.float32)
            o = ob if o is None else jnp.where(row_b == b, ob, o)
        o = o * (1.0 / den)
        lse = top * scale + jnp.log(den)
        for h in range(group):
            head = g * group + h
            side, hh = head // half_heads, lax.rem(head, half_heads)
            part = slice(h * rows, (h + 1) * rows)
            out[side, :, pl.ds(pl.multiple_of(hh * HD, HD), HD)] = o[part]
            lse_out[side] = jnp.where(lane == hh, lse[part], lse_out[side])


def prefix_kernel(chips, rows, groups, group, n_readers, block, owner_ref, readers, *refs):
    q_refs = refs[:chips]
    own_kv, mate_kv = refs[chips : chips + 2]
    outs = refs[chips + 2 : 2 * chips + 2]
    keys, values, q_all, q_rows, o_rows, lse_rows, o_all, kv_sems = refs[2 * chips + 2 :]
    me, owner = place(), owner_ref[0]
    scale = 1.0 / HD**0.5
    half = groups * group * HD
    cols = groups * HD
    part = lax.rem(me, 2) if own_kv.shape[2] > cols else 0

    @pl.when(me // 2 == owner // 2)
    def _():
        for kind, buf in ((0, keys), (1, values)):

            @pl.when(me == owner)
            def _():
                own_part = own_kv.at[kind, :, pl.ds(pl.multiple_of(part * cols, 128), cols)]
                pltpu.make_async_copy(own_part, buf, kv_sems.at[kind]).start()

            @pl.when(me != owner)
            def _():
                pltpu.make_async_copy(mate_kv.at[kind], buf, kv_sems.at[kind]).start()

        for d in range(chips):
            for s in range(2):
                q_all[2 * d + s] = q_refs[d][s].astype(jnp.float32)
        for j in range(n_readers):
            slot = jnp.bitwise_xor(readers[j], me)
            x = q_all[slot]
            for g in range(groups):
                for h in range(group):
                    first = (h * n_readers + j) * rows
                    col = (g * group + h) * HD
                    q_rows[g, first : first + rows, :] = x[:, col : col + HD]
        total = group * n_readers * rows
        blocks = total // block

        for kind, buf in ((0, keys), (1, values)):
            pltpu.make_async_copy(mate_kv.at[kind], buf, kv_sems.at[kind]).wait()
        for g in range(groups):

            @pl.loop(0, blocks)
            def _(i):
                part = pl.ds(pl.multiple_of(i * block, block), block)
                q = q_rows[g, part, :].astype(jnp.bfloat16)
                k = keys[:, g * HD : (g + 1) * HD]
                s = lax.dot_general(q, k, (((1,), (1,)), ((), ())), preferred_element_type=jnp.float32)
                top = jnp.max(s, axis=1, keepdims=True)
                p = jnp.exp2((s - top) * (scale * LOG2E))
                den = jnp.sum(p, axis=1, keepdims=True)
                v = values[:, g * HD : (g + 1) * HD]
                o = jnp.dot(p.astype(jnp.bfloat16), v, preferred_element_type=jnp.float32)
                o_rows[g, part, :] = o * (1.0 / den)
                lse_rows[g, part, :] = jnp.broadcast_to(top * scale + jnp.log(den), (block, 128))

        lane = lax.broadcasted_iota(jnp.int32, (rows, 128), 1)
        heads = groups * group
        for j in range(n_readers):
            slot = jnp.bitwise_xor(readers[j], me)
            stat = jnp.zeros((rows, 128), jnp.float32)
            for g in range(groups):
                for h in range(group):
                    first = (h * n_readers + j) * rows
                    hh = g * group + h
                    o_all[slot, :, hh * HD : (hh + 1) * HD] = o_rows[g, first : first + rows, :]
                    val = lse_rows[g, first : first + rows, :]
                    top = val.astype(jnp.bfloat16).astype(jnp.float32)
                    rest = val - top
                    mid = rest.astype(jnp.bfloat16).astype(jnp.float32)
                    stat = jnp.where(lane == hh, top, stat)
                    stat = jnp.where(lane == heads + hh, mid, stat)
                    stat = jnp.where(lane == 2 * heads + hh, rest - mid, stat)
            o_all[slot, :, half:] = stat
        for d in range(chips):
            for s in range(2):
                outs[d][s] = o_all[2 * d + s].astype(jnp.bfloat16)


def project(attn, w, first, count, out, col):
    width = w.shape[2]

    @pl.loop(0, count)
    def _(j):
        cols = pl.ds(pl.multiple_of(col + j * width, width), width)
        out[:, cols] = jnp.dot(attn[...], w[first + j], preferred_element_type=jnp.float32)


def away_kernel(heads, plan, readers, near, far, res, res_lse, w_hbm, w, *refs):
    n_tp, chunk, width = plan
    per_chunk = chunk // width
    outs, (attn, w_late, w_sems) = refs[: n_tp - 1], refs[n_tp - 1 :]
    copies = w_copies(plan, n_tp * per_chunk - w_late.shape[0], w_hbm, w_late, w_sems)
    for copy in copies:
        copy.start()
    me = place()
    core = lax.rem(me, 2)
    is_reader = jnp.int32(0)
    for j in range(readers.shape[0]):
        is_reader = jnp.where(readers[j] == me, 1, is_reader)
    half = heads * HD
    for side in range(2):
        mine = core == side
        stat = jnp.where(mine, near[:, half:].astype(jnp.float32), far[:, half:].astype(jnp.float32))
        pre = stat + pltpu.roll(stat, 128 - heads, 1) + pltpu.roll(stat, 128 - 2 * heads, 1)
        weights = 1.0 / (1.0 + jnp.exp(res_lse[side] - pre))
        for h in range(heads):
            weight = weights[:, h : h + 1]
            cols = slice(h * HD, (h + 1) * HD)
            r = res[side, :, cols]
            x = jnp.where(mine, near[:, cols].astype(jnp.float32), far[:, cols].astype(jnp.float32))
            y = jnp.where(is_reader > 0, r + weight * (x - r), r)
            attn[:, side * half + h * HD : side * half + (h + 1) * HD] = y.astype(jnp.bfloat16)
    for i, out in enumerate(outs):
        project(attn, w, i * per_chunk, per_chunk, out, 0)
    for copy in copies:
        copy.wait()


def home_kernel(attn, w, w_late, out):
    late = w_late.shape[0]
    early = out.shape[1] // w.shape[2] - late
    if early:
        project(attn, w, w.shape[0] - early, early, out, 0)
    project(attn, w_late, 0, late, out, early * w.shape[2])


def shards(n_dp, n_tp, queries, prefix_kv, cache_kv, lengths, page_table, owner, readers, w_out):
    rows = queries.shape[0]
    heads = queries.shape[1] // HD
    groups = prefix_kv.shape[2] // HD
    group = heads // groups
    prefix = prefix_kv.shape[1]
    maxpages = page_table.shape[1] // rows
    n_readers = readers.shape[0]
    chips = n_dp // 2
    half_groups = max(groups // 2, 1)
    half_heads = heads // 2
    share_group = half_heads // half_groups
    half = half_heads * HD
    wide = half + 128
    d_out = w_out.shape[1]
    chunk = d_out // n_tp

    def hop(x, d):
        return lax.ppermute(x, "dp", [(i, i ^ d) for i in range(n_dp)])

    mine, other = pl.pallas_call(
        functools.partial(split_kernel, half),
        out_shape=tuple(jax.ShapeDtypeStruct((rows, half), jnp.bfloat16) for _ in range(2)),
        in_specs=[vmem_spec()],
        out_specs=(vmem_spec(), vmem_spec()),
        compiler_params=pltpu.CompilerParams(vmem_limit_bytes=2 << 20),
        name="split",
    )(queries)
    got = hop(other, 1)
    kv_cols = half_groups * HD
    shared = pl.pallas_call(
        functools.partial(share_kernel, kv_cols),
        out_shape=jax.ShapeDtypeStruct((2, prefix, kv_cols), jnp.bfloat16),
        in_specs=[hbm_spec(), vmem_spec()],
        out_specs=vmem_spec(),
        scratch_shapes=[pltpu.SemaphoreType.DMA(())],
        compiler_params=pltpu.CompilerParams(vmem_limit_bytes=4 << 20),
        cost_estimate=pl.CostEstimate(flops=1 << 24, bytes_accessed=4 * prefix * kv_cols, transcendentals=0),
        name="share",
    )(in_hbm(prefix_kv), other)
    pair = pl.pallas_call(
        pair_kernel,
        out_shape=jax.ShapeDtypeStruct((2, rows, half), jnp.bfloat16),
        in_specs=[vmem_spec()] * 3,
        out_specs=vmem_spec(),
        compiler_params=pltpu.CompilerParams(vmem_limit_bytes=2 << 20),
        cost_estimate=pl.CostEstimate(flops=1 << 32, bytes_accessed=1 << 24, transcendentals=0),
        name="pair",
    )(mine, got, shared)
    width = min(512, chunk)
    plan = (n_tp, chunk, width)
    last = min(3, chunk // width)
    counts = (d_out // width - last, last)

    def w_blocks(n):
        return VMEM((n, w_out.shape[0], width), w_out.dtype)

    def with_chip(x, root, d):
        if root is None:
            return hop(x, 2 * d)
        pairs = []
        for i in range(n_dp):
            far = i ^ (2 * d)
            pairs.append((i, far if root in (i // 2, far // 2) else i ^ 1))
        return lax.ppermute(x, "dp", pairs)

    def gather(root, pair, shared, table, lengths, queries, cache_kv):
        got = [with_chip(pair, root, d) for d in range(1, chips)]
        mate_kv = hop(shared, 1)
        res, res_lse = pl.pallas_call(
            functools.partial(resident_kernel, rows, groups, group, maxpages),
            out_shape=(
                jax.ShapeDtypeStruct((2, rows, half), jnp.float32),
                jax.ShapeDtypeStruct((2, rows, 128), jnp.float32),
            ),
            in_specs=[smem_spec(), smem_spec(), vmem_spec(), hbm_spec()],
            out_specs=(vmem_spec(), vmem_spec()),
            scratch_shapes=[
                VMEM((rows, maxpages, PAGE, groups * HD), jnp.bfloat16),
                VMEM((rows, maxpages, PAGE, groups * HD), jnp.bfloat16),
                pltpu.SemaphoreType.DMA((2, rows)),
            ],
            compiler_params=pltpu.CompilerParams(vmem_limit_bytes=13 << 20),
            cost_estimate=pl.CostEstimate(
                flops=4 * heads * rows * rows * maxpages * PAGE * HD,
                bytes_accessed=2 * rows * maxpages * PAGE * groups * HD * 2,
                transcendentals=heads * rows * maxpages * PAGE,
            ),
            name="resident",
        )(table, lengths, queries, in_hbm(cache_kv))
        return (*got, mate_kv, res, res_lse)

    def finish(root, w_out, owner, readers, res, res_lse, *pre):
        back = [pre[0]] + [with_chip(pre[d], root, d) for d in range(1, chips)]
        loaded, token = pl.pallas_call(
            functools.partial(load_kernel, plan),
            out_shape=(w_blocks(counts[0]), jax.ShapeDtypeStruct((8, 128), jnp.float32)),
            in_specs=[hbm_spec(), vmem_spec()],
            out_specs=(vmem_spec(), vmem_spec()),
            scratch_shapes=[pltpu.SemaphoreType.DMA((counts[0],))],
            compiler_params=pltpu.CompilerParams(vmem_limit_bytes=2 << 20),
            cost_estimate=pl.CostEstimate(flops=1 << 28, bytes_accessed=w_out.size, transcendentals=0),
            name="load",
        )(in_hbm(w_out), pre[0])
        near, other = pl.pallas_call(
            functools.partial(choose_kernel, chips),
            out_shape=tuple(jax.ShapeDtypeStruct((rows, wide), jnp.bfloat16) for _ in range(2)),
            in_specs=[smem_spec()] + [vmem_spec()] * (chips + 1),
            out_specs=(vmem_spec(), vmem_spec()),
            compiler_params=pltpu.CompilerParams(vmem_limit_bytes=4 << 20),
            name="choose",
        )(owner, *back, token)
        far = hop(other, 1)
        in_vmem = functools.partial(pltpu.with_memory_space_constraint, memory_space=VMEM)
        cost = pl.CostEstimate(
            flops=2 * rows * heads * HD * chunk * 16, bytes_accessed=2 * heads * HD * chunk, transcendentals=0
        )
        *away, attn, late = pl.pallas_call(
            functools.partial(away_kernel, half_heads, plan),
            out_shape=tuple(jax.ShapeDtypeStruct((rows, chunk), jnp.float32) for _ in range(n_tp - 1))
            + (jax.ShapeDtypeStruct((rows, heads * HD), jnp.bfloat16), w_blocks(counts[1])),
            in_specs=[smem_spec()] + [vmem_spec()] * 4 + [hbm_spec(), vmem_spec()],
            out_specs=(vmem_spec(),) * (n_tp + 1),
            scratch_shapes=[pltpu.SemaphoreType.DMA((counts[1],))],
            compiler_params=pltpu.CompilerParams(vmem_limit_bytes=4 << 20),
            cost_estimate=cost,
            name="away",
        )(readers, near, far, res, res_lse, in_hbm(w_out), in_vmem(loaded))
        home = pl.pallas_call(
            home_kernel,
            out_shape=jax.ShapeDtypeStruct((rows, chunk), jnp.float32),
            in_specs=[vmem_spec()] * 3,
            out_specs=vmem_spec(),
            compiler_params=pltpu.CompilerParams(vmem_limit_bytes=4 << 20),
            cost_estimate=cost,
            name="home",
        )(attn, in_vmem(loaded), in_vmem(late))
        for k in range(1, n_tp):
            home = home + lax.ppermute(away[k - 1], "tp", [(i, i ^ k) for i in range(n_tp)])
        return home.astype(jnp.bfloat16)

    def routed(step, *operands):
        if chips > 8:
            return step(None, *operands)
        return lax.switch(owner[0] // 2, [functools.partial(step, k) for k in range(chips)], *operands)

    *gathered, mate_kv, res, res_lse = routed(gather, pair, shared, page_table[0], lengths, queries, cache_kv)
    gathered = [pair] + gathered
    total = share_group * n_readers * rows
    block = min(256, total)
    pre = pl.pallas_call(
        functools.partial(prefix_kernel, chips, rows, half_groups, share_group, n_readers, block),
        out_shape=tuple(jax.ShapeDtypeStruct((2, rows, wide), jnp.bfloat16) for _ in range(chips)),
        in_specs=[smem_spec(), smem_spec()] + [vmem_spec()] * chips + [hbm_spec()] * 2,
        out_specs=(vmem_spec(),) * chips,
        scratch_shapes=[
            VMEM((prefix, kv_cols), jnp.bfloat16),
            VMEM((prefix, kv_cols), jnp.bfloat16),
            VMEM((2 * chips, rows, half), jnp.float32),
            VMEM((half_groups, total, HD), jnp.float32),
            VMEM((half_groups, total, HD), jnp.float32),
            VMEM((half_groups, total, 128), jnp.float32),
            VMEM((2 * chips, rows, wide), jnp.float32),
            pltpu.SemaphoreType.DMA((2,)),
        ],
        compiler_params=pltpu.CompilerParams(vmem_limit_bytes=16 << 20),
        cost_estimate=pl.CostEstimate(
            flops=4 * half_groups * total * prefix * HD,
            bytes_accessed=4 * half_groups * prefix * HD,
            transcendentals=half_groups * total * prefix,
        ),
        name="prefix",
    )(owner, readers, *gathered, in_hbm(prefix_kv), in_hbm(mate_kv))
    return routed(finish, w_out, owner, readers, res, res_lse, *pre)


def solution(mesh):
    placed = (
        P("dp", "tp"),
        P(None, "dp", "tp"),
        P(None, "dp", None, "tp"),
        P("dp"),
        P("dp", None),
        P(),
        P(),
        P("tp", None),
    )
    return jax.shard_map(
        functools.partial(shards, mesh.shape["dp"], mesh.shape["tp"]),
        mesh=mesh,
        in_specs=placed,
        out_specs=P("dp", "tp"),
        check_vma=False,
    )
```

```python
import functools

import jax
import jax.numpy as jnp
from jax import lax
from jax.experimental import pallas as pl
from jax.experimental.pallas import tpu as pltpu
from jax.sharding import PartitionSpec as P


HD = 128
PAGE = 64
LOG2E = 1.4426950408889634
VMEM = pltpu.VMEM
SMEM = pltpu.SMEM


def vmem_spec():
    return pl.BlockSpec(memory_space=VMEM)


def smem_spec():
    return pl.BlockSpec(memory_space=SMEM)


def hbm_spec():
    return pl.BlockSpec(memory_space=pltpu.HBM)


def in_hbm(x):
    return pltpu.with_memory_space_constraint(x, pltpu.HBM)


def place():
    return lax.axis_index("dp").astype(jnp.int32)


def split_kernel(half, q_ref, mine, other, whole):
    whole[...] = q_ref[...]
    core = lax.rem(place(), 2)
    mine[...] = q_ref[:, pl.ds(pl.multiple_of(core * half, 128), half)]
    other[...] = q_ref[:, pl.ds(pl.multiple_of((1 - core) * half, 128), half)]


def pair_kernel(mine, got, after, out):
    out[0] = mine[...]
    out[1] = got[...]


def share_kernel(cols, kv, after, out, sem):
    side = 1 - lax.rem(place(), 2) if kv.shape[2] > cols else 0
    copy = pltpu.make_async_copy(kv.at[:, :, pl.ds(pl.multiple_of(side * cols, 128), cols)], out, sem)
    copy.start()
    copy.wait()


def w_copies(plan, first, w, outs, sems):
    n_tp, chunk, width = plan
    per_chunk = chunk // width
    my_tp = lax.axis_index("tp").astype(jnp.int32)
    copies = []
    for i in range(outs.shape[0]):
        which, block = divmod(first + i, per_chunk)
        col = jnp.bitwise_xor(my_tp, (which + 1) % n_tp) * chunk + block * width
        copies.append(pltpu.make_async_copy(w.at[:, pl.ds(pl.multiple_of(col, 128), width)], outs.at[i], sems.at[i]))
    return copies


def load_kernel(plan, w, after, out, token, sems):
    copies = w_copies(plan, 0, w, out, sems)
    for copy in copies:
        copy.start()
    for copy in copies:
        copy.wait()
    token[...] = jnp.zeros_like(token)


def choose_kernel(chips, root, *refs):
    if root is None:
        root, refs = refs[-3][0] // 2, refs[:-3] + refs[-2:]
    parts, near, far = refs[:chips], refs[chips + 1], refs[chips + 2]
    source = jnp.bitwise_xor(place() // 2, root)
    for d in range(chips):

        @pl.when(source == d)
        def _():
            near[...] = parts[d][0]
            far[...] = parts[d][1]


def resident_kernel(
    rows, groups, group, maxpages, table, lengths, q_ref, cache, out, lse_out, kbuf, vbuf, sems
):
    length = maxpages * PAGE
    scale = 1.0 / HD**0.5
    for kind, buf in ((0, kbuf), (1, vbuf)):
        for b in range(rows):
            for t in range(maxpages):
                pltpu.make_async_copy(
                    cache.at[kind, table[b * maxpages + t]], buf.at[b, t], sems.at[kind, b]
                ).start()
    m_rows = group * rows
    row_b = lax.rem(lax.broadcasted_iota(jnp.int32, (m_rows, 1), 0), rows)
    lens = jnp.zeros((m_rows, 1), jnp.int32)
    for b in range(rows):
        lens = jnp.where(row_b == b, lengths[b], lens)
    inside = lax.broadcasted_iota(jnp.int32, (m_rows, length), 1) < lens
    half_heads = groups * group // 2
    lane = lax.broadcasted_iota(jnp.int32, (rows, 128), 1)
    lse_out[...] = jnp.zeros_like(lse_out)

    def arrived(kind, buf):
        for b in range(rows):
            pltpu.make_async_copy(cache.at[kind, pl.ds(0, maxpages)], buf.at[b], sems.at[kind, b]).wait()

    arrived(0, kbuf)

    @pl.loop(0, groups)
    def _(g):
        kv_cols = pl.ds(pl.multiple_of(g * HD, HD), HD)
        q_cols = pl.ds(pl.multiple_of(g * group * HD, group * HD), group * HD)
        q = q_ref[:, q_cols].astype(jnp.float32)
        q = jnp.concatenate([q[:, h * HD : (h + 1) * HD] for h in range(group)], axis=0).astype(jnp.bfloat16)
        s = None
        for b in range(rows):
            keys = kbuf[b, :, :, kv_cols].reshape(length, HD)
            sb = lax.dot_general(q, keys, (((1,), (1,)), ((), ())), preferred_element_type=jnp.float32)
            s = sb if s is None else jnp.where(row_b == b, sb, s)
        s = jnp.where(inside, s, -jnp.inf)
        top = jnp.max(s, axis=1, keepdims=True)
        p = jnp.exp2((s - top) * (scale * LOG2E))
        den = jnp.sum(p, axis=1, keepdims=True)
        p = p.astype(jnp.bfloat16)

        @pl.when(g == 0)
        def _():
            arrived(1, vbuf)

        o = None
        for b in range(rows):
            values = vbuf[b, :, :, kv_cols].reshape(length, HD)
            ob = jnp.dot(p, values, preferred_element_type=jnp.float32)
            o = ob if o is None else jnp.where(row_b == b, ob, o)
        o = o * (1.0 / den)
        lse = top * scale + jnp.log(den)
        for h in range(group):
            head = g * group + h
            side, hh = head // half_heads, lax.rem(head, half_heads)
            part = slice(h * rows, (h + 1) * rows)
            out[side, :, pl.ds(pl.multiple_of(hh * HD, HD), HD)] = o[part]
            lse_out[side] = jnp.where(lane == hh, lse[part], lse_out[side])


def prefix_kernel(chips, rows, groups, group, n_readers, block, owner_ref, readers, *refs):
    q_refs = refs[:chips]
    own_kv, mate_kv = refs[chips : chips + 2]
    outs = refs[chips + 2 : 2 * chips + 2]
    keys, values, q_in, q_rows, o_rows, lse_rows, o_all, kv_sems, q_sems = refs[2 * chips + 2 :]
    me, owner = place(), owner_ref[0]
    scale = 1.0 / HD**0.5
    half = groups * group * HD
    cols = groups * HD
    part = lax.rem(me, 2) if own_kv.shape[2] > cols else 0

    @pl.when(me // 2 == owner // 2)
    def _():
        q_copies = [pltpu.make_async_copy(q_refs[d], q_in.at[d], q_sems.at[d]) for d in range(1, chips)]
        for kind, buf in ((0, keys), (1, values)):
            if kind:
                for copy in q_copies:
                    copy.start()

            @pl.when(me == owner)
            def _():
                own_part = own_kv.at[kind, :, pl.ds(pl.multiple_of(part * cols, 128), cols)]
                pltpu.make_async_copy(own_part, buf, kv_sems.at[kind]).start()

            @pl.when(me != owner)
            def _():
                pltpu.make_async_copy(mate_kv.at[kind], buf, kv_sems.at[kind]).start()

        q_in[0] = q_refs[0][...]
        for copy in q_copies:
            copy.wait()
        for j in range(n_readers):
            slot = jnp.bitwise_xor(readers[j], me)
            x = q_in[slot // 2, lax.rem(slot, 2)].astype(jnp.float32)
            for g in range(groups):
                for h in range(group):
                    first = (h * n_readers + j) * rows
                    col = (g * group + h) * HD
                    q_rows[g, first : first + rows, :] = x[:, col : col + HD]
        total = group * n_readers * rows
        blocks = total // block

        def arrived(kind, buf):
            pltpu.make_async_copy(mate_kv.at[kind], buf, kv_sems.at[kind]).wait()

        arrived(0, keys)
        for g in range(groups):
            for i in range(blocks):
                span = slice(i * block, (i + 1) * block)
                q = q_rows[g, span, :].astype(jnp.bfloat16)
                k = keys[:, g * HD : (g + 1) * HD]
                s = lax.dot_general(q, k, (((1,), (1,)), ((), ())), preferred_element_type=jnp.float32)
                top = jnp.max(s, axis=1, keepdims=True)
                p = jnp.exp2((s - top) * (scale * LOG2E))
                den = jnp.sum(p, axis=1, keepdims=True)
                if g == 0 and i == 0:
                    arrived(1, values)
                v = values[:, g * HD : (g + 1) * HD]
                o = jnp.dot(p.astype(jnp.bfloat16), v, preferred_element_type=jnp.float32)
                o_rows[g, span, :] = o * (1.0 / den)
                lse_rows[g, span, :] = jnp.broadcast_to(top * scale + jnp.log(den), (block, 128))

        lane = lax.broadcasted_iota(jnp.int32, (rows, 128), 1)
        heads = groups * group
        for slot in range(2 * chips):
            o_all[slot, :, half:] = jnp.zeros((rows, 128), jnp.float32)
        for j in range(n_readers):
            slot = jnp.bitwise_xor(readers[j], me)
            stat = jnp.where(lane == 127, 1.0, 0.0)
            for g in range(groups):
                for h in range(group):
                    first = (h * n_readers + j) * rows
                    hh = g * group + h
                    o_all[slot, :, hh * HD : (hh + 1) * HD] = o_rows[g, first : first + rows, :]
                    val = lse_rows[g, first : first + rows, :]
                    top = val.astype(jnp.bfloat16).astype(jnp.float32)
                    rest = val - top
                    mid = rest.astype(jnp.bfloat16).astype(jnp.float32)
                    stat = jnp.where(lane == hh, top, stat)
                    stat = jnp.where(lane == heads + hh, mid, stat)
                    stat = jnp.where(lane == 2 * heads + hh, rest - mid, stat)
            o_all[slot, :, half:] = stat
        for d in range(chips):
            for s in range(2):
                outs[d][s] = o_all[2 * d + s].astype(jnp.bfloat16)


def project(attn, w, first, count, out, col):
    width = w.shape[2]

    @pl.loop(0, count)
    def _(j):
        cols = pl.ds(pl.multiple_of(col + j * width, width), width)
        out[:, cols] = jnp.dot(attn[...], w[first + j], preferred_element_type=jnp.float32)


def merge(heads, core, part, res, res_lse, store):
    stat = part[:, heads * HD :].astype(jnp.float32)
    is_reader = stat[:, 127:128]
    pre = stat + pltpu.roll(stat, 128 - heads, 1) + pltpu.roll(stat, 128 - 2 * heads, 1)
    weights = 1.0 / (1.0 + jnp.exp(res_lse[core] - pre))
    for h in range(heads):
        cols = slice(h * HD, (h + 1) * HD)
        r = res[core, :, cols]
        y = r + weights[:, h : h + 1] * (part[:, cols].astype(jnp.float32) - r)
        store(h, jnp.where(is_reader > 0.5, y, r).astype(jnp.bfloat16))


def near_kernel(heads, part, res, res_lse, out):
    def store(h, x):
        out[:, h * HD : (h + 1) * HD] = x

    merge(heads, lax.rem(place(), 2), part, res, res_lse, store)


def away_kernel(heads, plan, near, far, res, res_lse, w_hbm, w, *refs):
    n_tp, chunk, width = plan
    per_chunk = chunk // width
    outs, (attn, w_late, w_sems) = refs[: n_tp - 1], refs[n_tp - 1 :]
    copies = w_copies(plan, n_tp * per_chunk - w_late.shape[0], w_hbm, w_late, w_sems)
    for copy in copies:
        copy.start()
    half = heads * HD
    core = lax.rem(place(), 2)
    attn[:, pl.ds(pl.multiple_of(core * half, half), half)] = near[...]

    def store(h, x):
        attn[:, pl.ds(pl.multiple_of((1 - core) * half + h * HD, HD), HD)] = x

    merge(heads, 1 - core, far, res, res_lse, store)
    for i, out in enumerate(outs):
        project(attn, w, i * per_chunk, per_chunk, out, 0)
    for copy in copies:
        copy.wait()


def home_kernel(attn, w, w_late, out):
    late = w_late.shape[0]
    early = out.shape[1] // w.shape[2] - late
    if early:
        project(attn, w, w.shape[0] - early, early, out, 0)
    project(attn, w_late, 0, late, out, early * w.shape[2])


def shards(n_dp, n_tp, queries, prefix_kv, cache_kv, lengths, page_table, owner, readers, w_out):
    rows = queries.shape[0]
    heads = queries.shape[1] // HD
    groups = prefix_kv.shape[2] // HD
    group = heads // groups
    prefix = prefix_kv.shape[1]
    maxpages = page_table.shape[1] // rows
    n_readers = readers.shape[0]
    chips = n_dp // 2
    half_groups = max(groups // 2, 1)
    half_heads = heads // 2
    share_group = half_heads // half_groups
    half = half_heads * HD
    wide = half + 128
    d_out = w_out.shape[1]
    chunk = d_out // n_tp

    def hop(x, d):
        return lax.ppermute(x, "dp", [(i, i ^ d) for i in range(n_dp)])

    mine, other, queries = pl.pallas_call(
        functools.partial(split_kernel, half),
        out_shape=tuple(jax.ShapeDtypeStruct((rows, n), jnp.bfloat16) for n in (half, half, 2 * half)),
        in_specs=[vmem_spec()],
        out_specs=(vmem_spec(),) * 3,
        compiler_params=pltpu.CompilerParams(vmem_limit_bytes=2 << 20),
        name="split",
    )(queries)
    got = hop(other, 1)
    kv_cols = half_groups * HD
    shared = pl.pallas_call(
        functools.partial(share_kernel, kv_cols),
        out_shape=jax.ShapeDtypeStruct((2, prefix, kv_cols), jnp.bfloat16),
        in_specs=[hbm_spec(), vmem_spec()],
        out_specs=vmem_spec(),
        scratch_shapes=[pltpu.SemaphoreType.DMA(())],
        compiler_params=pltpu.CompilerParams(vmem_limit_bytes=4 << 20),
        cost_estimate=pl.CostEstimate(flops=1 << 32, bytes_accessed=1 << 24, transcendentals=0),
        name="share",
    )(in_hbm(prefix_kv), other)
    pair = pl.pallas_call(
        pair_kernel,
        out_shape=jax.ShapeDtypeStruct((2, rows, half), jnp.bfloat16),
        in_specs=[vmem_spec()] * 3,
        out_specs=vmem_spec(),
        compiler_params=pltpu.CompilerParams(vmem_limit_bytes=2 << 20),
        name="pair",
    )(mine, got, shared)
    width = min(512, chunk)
    plan = (n_tp, chunk, width)
    last = min(2, chunk // width)
    counts = (d_out // width - last, last)

    def w_blocks(n):
        return VMEM((n, w_out.shape[0], width), w_out.dtype)

    def with_chip(x, root, d):
        if root is None:
            return hop(x, 2 * d)
        pairs = []
        for i in range(n_dp):
            far = i ^ (2 * d)
            pairs.append((i, far if root in (i // 2, far // 2) else i ^ 1))
        return lax.ppermute(x, "dp", pairs)

    def gather(root, pair, shared, table, lengths, queries, cache_kv):
        got = []
        for d in range(1, chips):
            got.append(with_chip(pair, root, d))
        mate_kv = hop(shared, 1)
        res, res_lse = pl.pallas_call(
            functools.partial(resident_kernel, rows, groups, group, maxpages),
            out_shape=(
                jax.ShapeDtypeStruct((2, rows, half), jnp.float32),
                jax.ShapeDtypeStruct((2, rows, 128), jnp.float32),
            ),
            in_specs=[smem_spec(), smem_spec(), vmem_spec(), hbm_spec()],
            out_specs=(vmem_spec(), vmem_spec()),
            scratch_shapes=[
                VMEM((rows, maxpages, PAGE, groups * HD), jnp.bfloat16),
                VMEM((rows, maxpages, PAGE, groups * HD), jnp.bfloat16),
                pltpu.SemaphoreType.DMA((2, rows)),
            ],
            compiler_params=pltpu.CompilerParams(vmem_limit_bytes=13 << 20),
            cost_estimate=pl.CostEstimate(
                flops=4 * heads * rows * rows * maxpages * PAGE * HD,
                bytes_accessed=2 * rows * maxpages * PAGE * groups * HD * 2,
                transcendentals=heads * rows * maxpages * PAGE,
            ),
            name="resident",
        )(table, lengths, queries, in_hbm(cache_kv))
        return (*got, mate_kv, res, res_lse)

    def finish(root, w_out, owner, res, res_lse, *pre):
        back = [pre[0]] + [with_chip(pre[d], root, d) for d in range(1, chips)]
        loaded, token = pl.pallas_call(
            functools.partial(load_kernel, plan),
            out_shape=(w_blocks(counts[0]), jax.ShapeDtypeStruct((8, 128), jnp.float32)),
            in_specs=[hbm_spec(), vmem_spec()],
            out_specs=(vmem_spec(), vmem_spec()),
            scratch_shapes=[pltpu.SemaphoreType.DMA((counts[0],))],
            compiler_params=pltpu.CompilerParams(vmem_limit_bytes=2 << 20),
            cost_estimate=pl.CostEstimate(flops=1 << 28, bytes_accessed=w_out.size, transcendentals=0),
            name="load",
        )(in_hbm(w_out), pre[0])
        near, other = pl.pallas_call(
            functools.partial(choose_kernel, chips, root),
            out_shape=tuple(jax.ShapeDtypeStruct((rows, wide), jnp.bfloat16) for _ in range(2)),
            in_specs=[vmem_spec()] * (chips + 1) + ([smem_spec()] if root is None else []),
            out_specs=(vmem_spec(), vmem_spec()),
            compiler_params=pltpu.CompilerParams(vmem_limit_bytes=4 << 20),
            name="choose",
        )(*back, token, *([owner] if root is None else []))
        far = hop(other, 1)
        near = pl.pallas_call(
            functools.partial(near_kernel, half_heads),
            out_shape=jax.ShapeDtypeStruct((rows, half), jnp.bfloat16),
            in_specs=[vmem_spec()] * 3,
            out_specs=vmem_spec(),
            compiler_params=pltpu.CompilerParams(vmem_limit_bytes=4 << 20),
            cost_estimate=pl.CostEstimate(flops=1 << 20, bytes_accessed=1 << 17, transcendentals=0),
            name="near",
        )(near, res, res_lse)
        in_vmem = functools.partial(pltpu.with_memory_space_constraint, memory_space=VMEM)
        cost = pl.CostEstimate(
            flops=2 * rows * heads * HD * chunk * 16, bytes_accessed=2 * heads * HD * chunk, transcendentals=0
        )
        *away, attn, late = pl.pallas_call(
            functools.partial(away_kernel, half_heads, plan),
            out_shape=tuple(jax.ShapeDtypeStruct((rows, chunk), jnp.float32) for _ in range(n_tp - 1))
            + (jax.ShapeDtypeStruct((rows, heads * HD), jnp.bfloat16), w_blocks(counts[1])),
            in_specs=[vmem_spec()] * 4 + [hbm_spec(), vmem_spec()],
            out_specs=(vmem_spec(),) * (n_tp + 1),
            scratch_shapes=[pltpu.SemaphoreType.DMA((counts[1],))],
            compiler_params=pltpu.CompilerParams(vmem_limit_bytes=4 << 20),
            cost_estimate=cost,
            name="away",
        )(near, far, res, res_lse, in_hbm(w_out), in_vmem(loaded))
        home = pl.pallas_call(
            home_kernel,
            out_shape=jax.ShapeDtypeStruct((rows, chunk), jnp.float32),
            in_specs=[vmem_spec()] * 3,
            out_specs=vmem_spec(),
            compiler_params=pltpu.CompilerParams(vmem_limit_bytes=4 << 20),
            cost_estimate=cost,
            name="home",
        )(attn, in_vmem(loaded), in_vmem(late))
        for k in range(1, n_tp):
            home = home + lax.ppermute(away[k - 1], "tp", [(i, i ^ k) for i in range(n_tp)])
        return home.astype(jnp.bfloat16)

    def routed(step, *operands):
        if chips > 8:
            return step(None, *operands)
        return lax.switch(lax.shift_right_logical(owner[0], 1), [functools.partial(step, k) for k in range(chips)], *operands)

    *gathered, mate_kv, res, res_lse = routed(gather, pair, shared, page_table[0], lengths, queries, cache_kv)
    gathered = [pair] + gathered
    total = share_group * n_readers * rows
    block = min(256, total)
    pre = pl.pallas_call(
        functools.partial(prefix_kernel, chips, rows, half_groups, share_group, n_readers, block),
        out_shape=tuple(jax.ShapeDtypeStruct((2, rows, wide), jnp.bfloat16) for _ in range(chips)),
        in_specs=[smem_spec(), smem_spec()] + [vmem_spec()] + [hbm_spec()] * (chips + 1),
        out_specs=(vmem_spec(),) * chips,
        scratch_shapes=[
            VMEM((prefix, kv_cols), jnp.bfloat16),
            VMEM((prefix, kv_cols), jnp.bfloat16),
            VMEM((chips, 2, rows, half), jnp.bfloat16),
            VMEM((half_groups, total, HD), jnp.float32),
            VMEM((half_groups, total, HD), jnp.float32),
            VMEM((half_groups, total, 128), jnp.float32),
            VMEM((2 * chips, rows, wide), jnp.float32),
            pltpu.SemaphoreType.DMA((2,)),
            pltpu.SemaphoreType.DMA((chips,)),
        ],
        compiler_params=pltpu.CompilerParams(vmem_limit_bytes=16 << 20),
        cost_estimate=pl.CostEstimate(
            flops=4 * half_groups * total * prefix * HD,
            bytes_accessed=4 * half_groups * prefix * HD,
            transcendentals=half_groups * total * prefix,
        ),
        name="prefix",
    )(owner, readers, gathered[0], *map(in_hbm, gathered[1:]), in_hbm(prefix_kv), in_hbm(mate_kv))
    return routed(finish, w_out, owner, res, res_lse, *pre)


def solution(mesh):
    placed = (
        P("dp", "tp"),
        P(None, "dp", "tp"),
        P(None, "dp", None, "tp"),
        P("dp"),
        P("dp", None),
        P(),
        P(),
        P("tp", None),
    )
    return jax.shard_map(
        functools.partial(shards, mesh.shape["dp"], mesh.shape["tp"]),
        mesh=mesh,
        in_specs=placed,
        out_specs=P("dp", "tp"),
        check_vma=False,
    )
```

```python
import functools

import jax
import jax.numpy as jnp
from jax import lax
from jax.experimental import pallas as pl
from jax.experimental.pallas import tpu as pltpu
from jax.sharding import PartitionSpec as P


HD = 128
PAGE = 64
PIECES = 4
LOG2E = 1.4426950408889634
VMEM = pltpu.VMEM
SMEM = pltpu.SMEM


def vmem_spec():
    return pl.BlockSpec(memory_space=VMEM)


def smem_spec():
    return pl.BlockSpec(memory_space=SMEM)


def hbm_spec():
    return pl.BlockSpec(memory_space=pltpu.HBM)


def in_hbm(x):
    return pltpu.with_memory_space_constraint(x, pltpu.HBM)


def place():
    return lax.axis_index("dp").astype(jnp.int32)


def split_kernel(half, q_ref, mine, other, whole):
    whole[...] = q_ref[...]
    core = lax.rem(place(), 2)
    mine[...] = q_ref[:, pl.ds(pl.multiple_of(core * half, 128), half)]
    other[...] = q_ref[:, pl.ds(pl.multiple_of((1 - core) * half, 128), half)]


def pair_kernel(mine, got, after, out):
    out[0] = mine[...]
    out[1] = got[...]


def piece(length, i):
    return pl.ds(i * (length // PIECES), length // PIECES)


def share_kernel(cols, kv, after, out, sems):
    side = 1 - lax.rem(place(), 2) if kv.shape[2] > cols else 0
    columns = pl.ds(pl.multiple_of(side * cols, 128), cols)
    copies = []
    for kind in range(2):
        for i in range(PIECES):
            span = piece(kv.shape[1], i)
            source, target = kv.at[kind, span, columns], out.at[kind, span]
            copies.append(pltpu.make_async_copy(source, target, sems.at[kind * PIECES + i]))
            copies[-1].start()
    for copy in copies:
        copy.wait()


def w_copies(plan, first, w, outs, sems):
    n_tp, chunk, width = plan
    per_chunk = chunk // width
    my_tp = lax.axis_index("tp").astype(jnp.int32)
    copies = []
    for i in range(outs.shape[0]):
        which, block = divmod(first + i, per_chunk)
        col = jnp.bitwise_xor(my_tp, (which + 1) % n_tp) * chunk + block * width
        copies.append(pltpu.make_async_copy(w.at[:, pl.ds(pl.multiple_of(col, 128), width)], outs.at[i], sems.at[i]))
    return copies


def load_kernel(plan, w, after, out, token, sems):
    copies = w_copies(plan, 0, w, out, sems)
    for copy in copies:
        copy.start()
    for copy in copies:
        copy.wait()
    token[...] = jnp.zeros_like(token)


def choose_kernel(chips, root, *refs):
    if root is None:
        root, refs = refs[-3][0] // 2, refs[:-3] + refs[-2:]
    parts, near, far = refs[:chips], refs[chips + 1], refs[chips + 2]
    source = jnp.bitwise_xor(place() // 2, root)
    for d in range(chips):

        @pl.when(source == d)
        def _():
            near[...] = parts[d][0]
            far[...] = parts[d][1]


def resident_kernel(
    rows, groups, group, maxpages, table, lengths, q_ref, cache, out, lse_out, kbuf, vbuf, sems
):
    length = maxpages * PAGE
    scale = 1.0 / HD**0.5
    for kind, buf in ((0, kbuf), (1, vbuf)):
        for b in range(rows):
            for t in range(maxpages):
                pltpu.make_async_copy(
                    cache.at[kind, table[b * maxpages + t]], buf.at[b, t], sems.at[kind, b]
                ).start()
    m_rows = group * rows
    row_b = lax.rem(lax.broadcasted_iota(jnp.int32, (m_rows, 1), 0), rows)
    lens = jnp.zeros((m_rows, 1), jnp.int32)
    for b in range(rows):
        lens = jnp.where(row_b == b, lengths[b], lens)
    inside = lax.broadcasted_iota(jnp.int32, (m_rows, length), 1) < lens
    half_heads = groups * group // 2
    lane = lax.broadcasted_iota(jnp.int32, (rows, 128), 1)
    lse_out[...] = jnp.zeros_like(lse_out)

    def arrived(kind, buf):
        for b in range(rows):
            pltpu.make_async_copy(cache.at[kind, pl.ds(0, maxpages)], buf.at[b], sems.at[kind, b]).wait()

    arrived(0, kbuf)

    @pl.loop(0, groups)
    def _(g):
        kv_cols = pl.ds(pl.multiple_of(g * HD, HD), HD)
        q_cols = pl.ds(pl.multiple_of(g * group * HD, group * HD), group * HD)
        q = q_ref[:, q_cols].astype(jnp.float32)
        q = jnp.concatenate([q[:, h * HD : (h + 1) * HD] for h in range(group)], axis=0).astype(jnp.bfloat16)
        s = None
        for b in range(rows):
            keys = kbuf[b, :, :, kv_cols].reshape(length, HD)
            sb = lax.dot_general(q, keys, (((1,), (1,)), ((), ())), preferred_element_type=jnp.float32)
            s = sb if s is None else jnp.where(row_b == b, sb, s)
        s = jnp.where(inside, s, -jnp.inf)
        top = jnp.max(s, axis=1, keepdims=True)
        p = jnp.exp2((s - top) * (scale * LOG2E))
        den = jnp.sum(p, axis=1, keepdims=True)
        p = p.astype(jnp.bfloat16)

        @pl.when(g == 0)
        def _():
            arrived(1, vbuf)

        o = None
        for b in range(rows):
            values = vbuf[b, :, :, kv_cols].reshape(length, HD)
            ob = jnp.dot(p, values, preferred_element_type=jnp.float32)
            o = ob if o is None else jnp.where(row_b == b, ob, o)
        o = o * (1.0 / den)
        lse = top * scale + jnp.log(den)
        for h in range(group):
            head = g * group + h
            side, hh = head // half_heads, lax.rem(head, half_heads)
            part = slice(h * rows, (h + 1) * rows)
            out[side, :, pl.ds(pl.multiple_of(hh * HD, HD), HD)] = o[part]
            lse_out[side] = jnp.where(lane == hh, lse[part], lse_out[side])


def prefix_kernel(chips, rows, groups, group, n_readers, block, owner_ref, readers, *refs):
    q_refs = refs[:chips]
    own_kv, mate_kv = refs[chips : chips + 2]
    outs = refs[chips + 2 : 2 * chips + 2]
    keys, values, q_in, q_rows, o_rows, lse_rows, o_all, kv_sems, q_sems = refs[2 * chips + 2 :]
    me, owner = place(), owner_ref[0]
    scale = 1.0 / HD**0.5
    half = groups * group * HD
    cols = groups * HD
    part = lax.rem(me, 2) if own_kv.shape[2] > cols else 0

    @pl.when(me // 2 == owner // 2)
    def _():
        q_copies = [pltpu.make_async_copy(q_refs[d], q_in.at[d], q_sems.at[d]) for d in range(1, chips)]
        for kind, buf in ((0, keys), (1, values)):
            if kind:
                for copy in q_copies:
                    copy.start()

            @pl.when(me == owner)
            def _():
                own_part = own_kv.at[kind, :, pl.ds(pl.multiple_of(part * cols, 128), cols)]
                pltpu.make_async_copy(own_part, buf, kv_sems.at[kind]).start()

            @pl.when(me != owner)
            def _():
                pltpu.make_async_copy(mate_kv.at[kind], buf, kv_sems.at[kind]).start()

        q_in[0] = q_refs[0][...]
        for copy in q_copies:
            copy.wait()
        for j in range(n_readers):
            slot = jnp.bitwise_xor(readers[j], me)
            x = q_in[slot // 2, lax.rem(slot, 2)].astype(jnp.float32)
            for g in range(groups):
                for h in range(group):
                    first = (h * n_readers + j) * rows
                    col = (g * group + h) * HD
                    q_rows[g, first : first + rows, :] = x[:, col : col + HD]
        total = group * n_readers * rows
        blocks = total // block

        def arrived(kind, buf):
            pltpu.make_async_copy(mate_kv.at[kind], buf, kv_sems.at[kind]).wait()

        arrived(0, keys)
        for g in range(groups):
            for i in range(blocks):
                span = slice(i * block, (i + 1) * block)
                q = q_rows[g, span, :].astype(jnp.bfloat16)
                k = keys[:, g * HD : (g + 1) * HD]
                s = lax.dot_general(q, k, (((1,), (1,)), ((), ())), preferred_element_type=jnp.float32)
                top = jnp.max(s, axis=1, keepdims=True)
                p = jnp.exp2((s - top) * (scale * LOG2E))
                den = jnp.sum(p, axis=1, keepdims=True)
                if g == 0 and i == 0:
                    arrived(1, values)
                v = values[:, g * HD : (g + 1) * HD]
                o = jnp.dot(p.astype(jnp.bfloat16), v, preferred_element_type=jnp.float32)
                o_rows[g, span, :] = o * (1.0 / den)
                lse_rows[g, span, :] = jnp.broadcast_to(top * scale + jnp.log(den), (block, 128))

        lane = lax.broadcasted_iota(jnp.int32, (rows, 128), 1)
        heads = groups * group
        for slot in range(2 * chips):
            o_all[slot, :, half:] = jnp.zeros((rows, 128), jnp.float32)
        for j in range(n_readers):
            slot = jnp.bitwise_xor(readers[j], me)
            stat = jnp.where(lane == 127, 1.0, 0.0)
            for g in range(groups):
                for h in range(group):
                    first = (h * n_readers + j) * rows
                    hh = g * group + h
                    o_all[slot, :, hh * HD : (hh + 1) * HD] = o_rows[g, first : first + rows, :]
                    val = lse_rows[g, first : first + rows, :]
                    top = val.astype(jnp.bfloat16).astype(jnp.float32)
                    rest = val - top
                    mid = rest.astype(jnp.bfloat16).astype(jnp.float32)
                    stat = jnp.where(lane == hh, top, stat)
                    stat = jnp.where(lane == heads + hh, mid, stat)
                    stat = jnp.where(lane == 2 * heads + hh, rest - mid, stat)
            o_all[slot, :, half:] = stat
        for d in range(chips):
            for s in range(2):
                outs[d][s] = o_all[2 * d + s].astype(jnp.bfloat16)


def project(attn, w, first, count, out, col):
    width = w.shape[2]

    @pl.loop(0, count)
    def _(j):
        cols = pl.ds(pl.multiple_of(col + j * width, width), width)
        out[:, cols] = jnp.dot(attn[...], w[first + j], preferred_element_type=jnp.float32)


def merge(heads, core, part, res, res_lse, store):
    stat = part[:, heads * HD :].astype(jnp.float32)
    is_reader = stat[:, 127:128]
    pre = stat + pltpu.roll(stat, 128 - heads, 1) + pltpu.roll(stat, 128 - 2 * heads, 1)
    weights = 1.0 / (1.0 + jnp.exp(res_lse[core] - pre))
    for h in range(heads):
        cols = slice(h * HD, (h + 1) * HD)
        r = res[core, :, cols]
        y = r + weights[:, h : h + 1] * (part[:, cols].astype(jnp.float32) - r)
        store(h, jnp.where(is_reader > 0.5, y, r).astype(jnp.bfloat16))


def near_kernel(heads, part, res, res_lse, out):
    def store(h, x):
        out[:, h * HD : (h + 1) * HD] = x

    merge(heads, lax.rem(place(), 2), part, res, res_lse, store)


def away_kernel(heads, plan, near, far, res, res_lse, w_hbm, w, *refs):
    n_tp, chunk, width = plan
    per_chunk = chunk // width
    outs, (attn, w_late, w_sems) = refs[: n_tp - 1], refs[n_tp - 1 :]
    copies = w_copies(plan, w.shape[0], w_hbm, w_late, w_sems)
    for copy in copies:
        copy.start()
    half = heads * HD
    core = lax.rem(place(), 2)
    attn[:, pl.ds(pl.multiple_of(core * half, half), half)] = near[...]

    def store(h, x):
        attn[:, pl.ds(pl.multiple_of((1 - core) * half + h * HD, HD), HD)] = x

    merge(heads, 1 - core, far, res, res_lse, store)
    for i, out in enumerate(outs):
        project(attn, w, i * per_chunk, per_chunk, out, 0)
    for copy in copies:
        copy.wait()


def home_kernel(plan, attn, w, w_late, w_hbm, out, w_last, w_sems):
    n_tp, chunk, width = plan
    late, last = w_late.shape[0], w_last.shape[0]
    copies = w_copies(plan, n_tp * (chunk // width) - last, w_hbm, w_last, w_sems)
    for copy in copies:
        copy.start()
    early = max(chunk // width - late - last, 0)
    if early:
        project(attn, w, w.shape[0] - early, early, out, 0)
    if chunk // width > last:
        project(attn, w_late, 0, late, out, early * width)
    for copy in copies:
        copy.wait()
    project(attn, w_last, 0, last, out, chunk - last * width)


def shards(n_dp, n_tp, queries, prefix_kv, cache_kv, lengths, page_table, owner, readers, w_out):
    rows = queries.shape[0]
    heads = queries.shape[1] // HD
    groups = prefix_kv.shape[2] // HD
    group = heads // groups
    prefix = prefix_kv.shape[1]
    maxpages = page_table.shape[1] // rows
    n_readers = readers.shape[0]
    chips = n_dp // 2
    half_groups = max(groups // 2, 1)
    half_heads = heads // 2
    share_group = half_heads // half_groups
    half = half_heads * HD
    wide = half + 128
    d_out = w_out.shape[1]
    chunk = d_out // n_tp

    def hop(x, d):
        return lax.ppermute(x, "dp", [(i, i ^ d) for i in range(n_dp)])

    mine, other, queries = pl.pallas_call(
        functools.partial(split_kernel, half),
        out_shape=tuple(jax.ShapeDtypeStruct((rows, n), jnp.bfloat16) for n in (half, half, 2 * half)),
        in_specs=[vmem_spec()],
        out_specs=(vmem_spec(),) * 3,
        compiler_params=pltpu.CompilerParams(vmem_limit_bytes=2 << 20),
        name="split",
    )(queries)
    got = hop(other, 1)
    kv_cols = half_groups * HD
    shared = pl.pallas_call(
        functools.partial(share_kernel, kv_cols),
        out_shape=jax.ShapeDtypeStruct((2, prefix, kv_cols), jnp.bfloat16),
        in_specs=[hbm_spec(), vmem_spec()],
        out_specs=vmem_spec(),
        scratch_shapes=[pltpu.SemaphoreType.DMA((2 * PIECES,))],
        compiler_params=pltpu.CompilerParams(vmem_limit_bytes=4 << 20),
        cost_estimate=pl.CostEstimate(flops=1 << 32, bytes_accessed=1 << 24, transcendentals=0),
        name="share",
    )(in_hbm(prefix_kv), other)
    pair = pl.pallas_call(
        pair_kernel,
        out_shape=jax.ShapeDtypeStruct((2, rows, half), jnp.bfloat16),
        in_specs=[vmem_spec()] * 3,
        out_specs=vmem_spec(),
        compiler_params=pltpu.CompilerParams(vmem_limit_bytes=2 << 20),
        name="pair",
    )(mine, got, shared)
    width = min(512, chunk)
    plan = (n_tp, chunk, width)
    blocks = d_out // width
    counts = (blocks - 2, 1, 1) if chunk // width > 2 else (blocks - 1, 1, 1)

    def w_blocks(n):
        return VMEM((n, w_out.shape[0], width), w_out.dtype)

    def with_chip(x, root, d):
        if root is None:
            return hop(x, 2 * d)
        pairs = []
        for i in range(n_dp):
            far = i ^ (2 * d)
            pairs.append((i, far if root in (i // 2, far // 2) else i ^ 1))
        return lax.ppermute(x, "dp", pairs)

    def gather(root, pair, shared, table, lengths, queries, cache_kv):
        got = []
        for d in range(1, chips):
            got.append(with_chip(pair, root, d))
        mate_kv = hop(shared, 1)
        res, res_lse = pl.pallas_call(
            functools.partial(resident_kernel, rows, groups, group, maxpages),
            out_shape=(
                jax.ShapeDtypeStruct((2, rows, half), jnp.float32),
                jax.ShapeDtypeStruct((2, rows, 128), jnp.float32),
            ),
            in_specs=[smem_spec(), smem_spec(), vmem_spec(), hbm_spec()],
            out_specs=(vmem_spec(), vmem_spec()),
            scratch_shapes=[
                VMEM((rows, maxpages, PAGE, groups * HD), jnp.bfloat16),
                VMEM((rows, maxpages, PAGE, groups * HD), jnp.bfloat16),
                pltpu.SemaphoreType.DMA((2, rows)),
            ],
            compiler_params=pltpu.CompilerParams(vmem_limit_bytes=13 << 20),
            cost_estimate=pl.CostEstimate(
                flops=4 * heads * rows * rows * maxpages * PAGE * HD,
                bytes_accessed=2 * rows * maxpages * PAGE * groups * HD * 2,
                transcendentals=heads * rows * maxpages * PAGE,
            ),
            name="resident",
        )(table, lengths, queries, in_hbm(cache_kv))
        return (*got, mate_kv, res, res_lse)

    def finish(root, w_out, owner, res, res_lse, *pre):
        back = [pre[0]] + [with_chip(pre[d], root, d) for d in range(1, chips)]
        loaded, token = pl.pallas_call(
            functools.partial(load_kernel, plan),
            out_shape=(w_blocks(counts[0]), jax.ShapeDtypeStruct((8, 128), jnp.float32)),
            in_specs=[hbm_spec(), vmem_spec()],
            out_specs=(vmem_spec(), vmem_spec()),
            scratch_shapes=[pltpu.SemaphoreType.DMA((counts[0],))],
            compiler_params=pltpu.CompilerParams(vmem_limit_bytes=2 << 20),
            cost_estimate=pl.CostEstimate(flops=1 << 28, bytes_accessed=w_out.size, transcendentals=0),
            name="load",
        )(in_hbm(w_out), pre[0])
        near, other = pl.pallas_call(
            functools.partial(choose_kernel, chips, root),
            out_shape=tuple(jax.ShapeDtypeStruct((rows, wide), jnp.bfloat16) for _ in range(2)),
            in_specs=[vmem_spec()] * (chips + 1) + ([smem_spec()] if root is None else []),
            out_specs=(vmem_spec(), vmem_spec()),
            compiler_params=pltpu.CompilerParams(vmem_limit_bytes=4 << 20),
            name="choose",
        )(*back, token, *([owner] if root is None else []))
        far = hop(other, 1)
        near = pl.pallas_call(
            functools.partial(near_kernel, half_heads),
            out_shape=jax.ShapeDtypeStruct((rows, half), jnp.bfloat16),
            in_specs=[vmem_spec()] * 3,
            out_specs=vmem_spec(),
            compiler_params=pltpu.CompilerParams(vmem_limit_bytes=4 << 20),
            cost_estimate=pl.CostEstimate(flops=1 << 20, bytes_accessed=1 << 17, transcendentals=0),
            name="near",
        )(near, res, res_lse)
        in_vmem = functools.partial(pltpu.with_memory_space_constraint, memory_space=VMEM)
        cost = pl.CostEstimate(
            flops=2 * rows * heads * HD * chunk * 16, bytes_accessed=2 * heads * HD * chunk, transcendentals=0
        )
        *away, attn, late = pl.pallas_call(
            functools.partial(away_kernel, half_heads, plan),
            out_shape=tuple(jax.ShapeDtypeStruct((rows, chunk), jnp.float32) for _ in range(n_tp - 1))
            + (jax.ShapeDtypeStruct((rows, heads * HD), jnp.bfloat16), w_blocks(counts[1])),
            in_specs=[vmem_spec()] * 4 + [hbm_spec(), vmem_spec()],
            out_specs=(vmem_spec(),) * (n_tp + 1),
            scratch_shapes=[pltpu.SemaphoreType.DMA((counts[1],))],
            compiler_params=pltpu.CompilerParams(vmem_limit_bytes=4 << 20),
            cost_estimate=cost,
            name="away",
        )(near, far, res, res_lse, in_hbm(w_out), in_vmem(loaded))
        home = pl.pallas_call(
            functools.partial(home_kernel, plan),
            out_shape=jax.ShapeDtypeStruct((rows, chunk), jnp.float32),
            in_specs=[vmem_spec()] * 3 + [hbm_spec()],
            out_specs=vmem_spec(),
            scratch_shapes=[
                VMEM((counts[2], w_out.shape[0], width), w_out.dtype),
                pltpu.SemaphoreType.DMA((counts[2],)),
            ],
            compiler_params=pltpu.CompilerParams(vmem_limit_bytes=8 << 20),
            cost_estimate=cost,
            name="home",
        )(attn, in_vmem(loaded), in_vmem(late), in_hbm(w_out))
        for k in range(1, n_tp):
            home = home + lax.ppermute(away[k - 1], "tp", [(i, i ^ k) for i in range(n_tp)])
        return home.astype(jnp.bfloat16)

    def routed(step, *operands):
        if chips > 8:
            return step(None, *operands)
        return lax.switch(lax.shift_right_logical(owner[0], 1), [functools.partial(step, k) for k in range(chips)], *operands)

    *gathered, mate_kv, res, res_lse = routed(gather, pair, shared, page_table[0], lengths, queries, cache_kv)
    gathered = [pair] + gathered
    total = share_group * n_readers * rows
    block = min(256, total)
    pre = pl.pallas_call(
        functools.partial(prefix_kernel, chips, rows, half_groups, share_group, n_readers, block),
        out_shape=tuple(jax.ShapeDtypeStruct((2, rows, wide), jnp.bfloat16) for _ in range(chips)),
        in_specs=[smem_spec(), smem_spec()] + [vmem_spec()] + [hbm_spec()] * (chips + 1),
        out_specs=(vmem_spec(),) * chips,
        scratch_shapes=[
            VMEM((prefix, kv_cols), jnp.bfloat16),
            VMEM((prefix, kv_cols), jnp.bfloat16),
            VMEM((chips, 2, rows, half), jnp.bfloat16),
            VMEM((half_groups, total, HD), jnp.float32),
            VMEM((half_groups, total, HD), jnp.float32),
            VMEM((half_groups, total, 128), jnp.float32),
            VMEM((2 * chips, rows, wide), jnp.float32),
            pltpu.SemaphoreType.DMA((2,)),
            pltpu.SemaphoreType.DMA((chips,)),
        ],
        compiler_params=pltpu.CompilerParams(vmem_limit_bytes=16 << 20),
        cost_estimate=pl.CostEstimate(
            flops=4 * half_groups * total * prefix * HD,
            bytes_accessed=4 * half_groups * prefix * HD,
            transcendentals=half_groups * total * prefix,
        ),
        name="prefix",
    )(owner, readers, gathered[0], *map(in_hbm, gathered[1:]), in_hbm(prefix_kv), in_hbm(mate_kv))
    return routed(finish, w_out, owner, res, res_lse, *pre)


def solution(mesh):
    placed = (
        P("dp", "tp"),
        P(None, "dp", "tp"),
        P(None, "dp", None, "tp"),
        P("dp"),
        P("dp", None),
        P(),
        P(),
        P("tp", None),
    )
    return jax.shard_map(
        functools.partial(shards, mesh.shape["dp"], mesh.shape["tp"]),
        mesh=mesh,
        in_specs=placed,
        out_specs=P("dp", "tp"),
        check_vma=False,
    )
```
